256 devices in a mesh: dp: 32 (over y, z_lo, x), tensor: 8 (over z_hi, core).
Axes of the slice: x: 4, y: 4, z: 8 (z_hi: 4, z_lo: 2; z = z_hi * 2 + z_lo), core: 2. Of those that a mesh axis runs over, the one named last changes fastest.
Arguments:
- hidden: bfloat16 [32768, 7168], P('dp', 'tensor'), parts along dimension 0, may hold values from -6 to 6
- w_dq: bfloat16 [7168, 1536], P('tensor'), may hold values from -0.0625 to 0.0625
- w_dkv: bfloat16 [7168, 576], P('tensor'), may hold values from -0.0625 to 0.0625
- q_gain: float32 [1536], replicated, may hold values from 0.1 to 1.9
- kv_gain: float32 [512], replicated, may hold values from 0.1 to 1.9
- w_uq: bfloat16 [1536, 12288], P(None, 'tensor'), may hold values from -0.15625 to 0.15625
- w_ukv: bfloat16 [512, 16384], P(None, 'tensor'), may hold values from -0.25 to 0.25
Outputs:
- queries: bfloat16 [32768, 12288], P('dp', 'tensor'), parts along dimension 0
- keys_values: bfloat16 [32768, 16384], P('dp', 'tensor'), parts along dimension 0
- rotary_key: bfloat16 [32768, 64], P(('dp', 'tensor')), parts along dimension 0
The draws below stay inside these ranges and needn't reach their ends.
There are 32 independent parts, one for each index of `dp`. The reference program is written for one: setup_inputs(seed, part) draws one part's arguments, and reference() takes and returns one part's arrays. A program takes and returns all parts, laid end to end along the dimension named above; an argument that names none is the same for every part. Nothing has to cross between parts.
All inputs are finite; a program needn't handle non-finite values.
Results may differ from the reference program's by a relative error of at most 0.0049.
Values may be sent and summed in bfloat16 or wider, within the bound.
A program may use at most 128 MiB of HBM per device.

```python
import jax
import jax.numpy as jnp
from jax import lax

D = 7168
QL = 1536
KL = 512
HEADS = 64
NOPE = 128
ROPE = 64
VDIM = 128
TOK = 1024


def block_scale(own_key, shape, split, least, top_value):
    level = 1.0
    for dim, shards_of in split:
        draws = jax.random.uniform(jax.random.fold_in(jax.random.fold_in(own_key, 6), dim), (shards_of,), jnp.float32, least / len(split), top_value / len(split))
        level = level * jnp.repeat(jnp.exp(draws), shape[dim] // shards_of).reshape((-1,) + (1,) * (len(shape) - 1 - dim))
    return level


def scatter_about(rng, dims, spread, most, shards=(), kind=jnp.bfloat16):
    result = jax.random.normal(rng, dims, jnp.float32) * spread
    if len(shards) > 0:
        result = block_scale(rng, dims, shards, -0.22, 0.18) * result
    return jnp.clip(result, min=-most, max=most).astype(kind)


def setup_inputs(seed: int = 0, part: int = 0) -> dict:
    seeds = jax.random.split(jax.random.key(seed), 8)
    part_keys = jax.random.split(jax.random.fold_in(seeds[7], part), 8)
    hidden = scatter_about(part_keys[0], (TOK, D), 1.0, 6.0, ((1, 8),))
    w_dq = scatter_about(seeds[1], (D, QL), D ** -0.5, 0.0625, ((0, 8),))
    w_dkv = scatter_about(seeds[2], (D, KL + ROPE), D ** -0.5, 0.0625, ((0, 8),))
    q_gain = jnp.clip(1.0 + 0.18 * jax.random.normal(seeds[3], (QL,), jnp.float32), 0.1, 1.9)
    kv_gain = jnp.clip(1.0 + 0.18 * jax.random.normal(seeds[4], (KL,), jnp.float32), 0.1, 1.9)
    w_uq = scatter_about(seeds[5], (QL, HEADS * (NOPE + ROPE)), QL ** -0.5, 0.15625, ((1, 8),))
    w_ukv = scatter_about(seeds[6], (KL, HEADS * (NOPE + VDIM)), KL ** -0.5, 0.25, ((1, 8),))
    return dict(hidden=hidden, w_dq=w_dq, w_dkv=w_dkv, q_gain=q_gain, kv_gain=kv_gain, w_uq=w_uq, w_ukv=w_ukv)


def rotate(values, angle):
    half = values.shape[-1] // 2
    first = values[..., :half]
    second = values[..., half:]
    cosine = jnp.cos(angle)
    sine = jnp.sin(angle)
    return jnp.concatenate([first * cosine - second * sine, second * cosine + first * sine], axis=-1)

def angles(positions, half):
    freqs = 50000.0 ** (-jnp.arange(half, dtype=jnp.float32) / half)
    return positions[:, None] * freqs[None, :]

def normalize(block, gain):
    scale = lax.rsqrt(lax.optimization_barrier(jnp.mean(block * block, axis=1, keepdims=True)) + 1e-06)
    return (block * scale * gain[None, :]).astype(jnp.bfloat16)

def reference(hidden, w_dq, w_dkv, q_gain, kv_gain, w_uq, w_ukv):
    down = jnp.concatenate([jnp.dot(hidden, w_dq, preferred_element_type=jnp.float32), jnp.dot(hidden, w_dkv, preferred_element_type=jnp.float32)], axis=1)
    q_latent = normalize(down[:, :QL], q_gain)
    kv_latent = normalize(down[:, QL:QL + KL], kv_gain)
    positions = jnp.arange(TOK, dtype=jnp.float32)
    angle = angles(positions, ROPE // 2)
    rotary_key = rotate(down[:, QL + KL:], angle).astype(jnp.bfloat16)
    query_full = jnp.dot(q_latent, w_uq, preferred_element_type=jnp.float32)
    query_full = query_full.reshape(TOK, HEADS, NOPE + ROPE)
    turned = rotate(query_full[:, :, NOPE:], angle[:, None, :])
    queries = jnp.concatenate([query_full[:, :, :NOPE], turned], axis=2)
    queries = queries.reshape(TOK, HEADS * (NOPE + ROPE)).astype(jnp.bfloat16)
    keys_values = jnp.dot(kv_latent, w_ukv, preferred_element_type=jnp.float32).astype(jnp.bfloat16)
    return (queries, keys_values, rotary_key)
```

```python
import functools

import jax
import jax.numpy as jnp
import numpy as np
from jax import lax
from jax.experimental import pallas as pl
from jax.experimental.pallas import tpu as pltpu
from jax.sharding import PartitionSpec as P

NOPE = 128
ROPE = 64
CHIPS = 4
PIECES = 4
MESH = pl.DeviceIdType.MESH
F32 = jnp.float32
BF16 = jnp.bfloat16


def rotary_tables(count):
    half = ROPE // 2
    freqs = (50000.0 ** (-np.arange(half, dtype=np.float32) / half)).astype(np.float32)
    angle = np.arange(count, dtype=np.float32)[:, None] * freqs[None, :]
    cosine = np.cos(angle.astype(np.float64)).astype(np.float32)
    sine = np.sin(angle.astype(np.float64)).astype(np.float32)
    cosine = np.tile(cosine, (1, 4))
    sine = np.concatenate([-sine, sine, -sine, sine], axis=1)
    return np.stack([cosine, sine])


def kernel(
    hidden, w_dq, w_dkv, q_gain, kv_gain, w_uq, w_ukv, table,
    q_out, kv_out, key_out,
    hid, wdq, wdkv, qg, kvg, wuq, wukv, tab,
    acc, pair_out, pair_in, ring_out, ring_in, lat, qbuf, kvbuf, keybuf,
    load_sem, pair_s, pair_r, rs_s, rs_r, ag_s, ag_r, fw_s, fw_r, out_sem,
):
    rows = hid.shape[0]
    q_width = wdq.shape[1]
    kv_width = kvg.shape[1]
    down_width = q_width + wdkv.shape[1]
    latent_width = q_width + kv_width
    block = rows // (2 * CHIPS)
    half = block // 2
    piece = half // PIECES
    me = lax.axis_index("tensor")
    chip = me // 2
    core = me - 2 * chip
    partner = me + 1 - 2 * core

    def chip_at(j):
        return lax.rem(chip + j, CHIPS)

    neighbour = (chip_at(1) * 2 + core, chip_at(CHIPS - 1) * 2 + core)
    toward = (1, CHIPS - 1)
    behind = (CHIPS - 1, 1)
    opposite = 2

    def load(i, src, dst):
        return pltpu.make_async_copy(src, dst, load_sem.at[i])

    def chip_rows(j):
        return pl.ds(pl.multiple_of(chip_at(j) * 2 * block, 2 * block), 2 * block)

    hid_loads = [load(j, hidden.at[chip_rows(j)], hid.at[chip_rows(j)]) for j in range(CHIPS)]
    first_loads = [load(4, w_dq, wdq), load(5, w_dkv, wdkv)]
    late_loads = [
        load(6, q_gain, qg), load(7, kv_gain, kvg), load(8, table, tab),
        load(9, w_uq, wuq), load(10, w_ukv, wukv),
    ]
    hid_loads[opposite].start()
    for copy in first_loads:
        copy.start()
    for j in (1, 3, 0):
        hid_loads[j].start()

    barrier = pltpu.get_barrier_semaphore()
    for device in (*neighbour, partner):
        pl.semaphore_signal(barrier, inc=1, device_id={"tensor": device}, device_id_type=MESH)

    def remote(src, dst, send, recv, device):
        return pltpu.make_async_remote_copy(
            src_ref=src, dst_ref=dst, send_sem=send, recv_sem=recv,
            device_id={"tensor": device}, device_id_type=MESH,
        )

    def down(j):
        base = chip_at(j) * 2 * block
        other = pl.ds(pl.multiple_of(base + (1 - core) * block, block), block)
        own = pl.ds(pl.multiple_of(base + core * block, block), block)

        def emit(start, width, weights):
            x = jnp.concatenate([hid[other, :], hid[own, :]], axis=0)
            r = jnp.dot(x, weights, preferred_element_type=F32)
            pair_out[j, :, pl.ds(start, width)] = r[:block].astype(BF16)
            acc[j, :, pl.ds(start, width)] = r[block:]

        @pl.loop(0, 3)
        def _(i):
            start = pl.multiple_of(i * (q_width // 3), 128)
            emit(start, q_width // 3, wdq[:, pl.ds(start, q_width // 3)])

        emit(q_width, kv_width, wdkv[:, :kv_width])
        emit(latent_width, ROPE, wdkv[:, kv_width:])

    pair_copies = [
        remote(pair_out.at[j], pair_in.at[j], pair_s.at[j], pair_r.at[j], partner)
        for j in range(CHIPS)
    ]

    def piece_rows(h, p):
        return pl.ds(h * half + p * piece, piece)

    def chip_sum(j, h, p):
        return acc[j, piece_rows(h, p), :] + pair_in[j, piece_rows(h, p), :].astype(F32)

    def ring_copy(d, stage, p):
        at = pl.ds(p * piece, piece)
        return remote(
            ring_out.at[d, stage, at], ring_in.at[d, stage, at],
            rs_s.at[d, stage, p], rs_r.at[d, stage, p], neighbour[d],
        )

    def ring_got(d, stage, p):
        return ring_in[d, stage, pl.ds(p * piece, piece), :].astype(F32)

    def ring_put(d, stage, p, value):
        ring_out[d, stage, pl.ds(p * piece, piece), :] = value.astype(BF16)

    def lat_rows(j, c, h, p):
        start = (chip_at(j) * 2 + c) * block + h * half + p * piece
        return pl.ds(pl.multiple_of(start, piece), piece)

    def gather_copy(d, stage, p):
        j = (0, 0, behind[d])[stage]
        h = (d, 1 - d, d)[stage]
        at = lat.at[lat_rows(j, core, h, p)]
        return remote(at, at, ag_s.at[d, stage, p], ag_r.at[d, stage, p], neighbour[d])

    def gather_wait(d, stage, p):
        j = (behind[d], behind[d], opposite)[stage]
        h = (d, 1 - d, d)[stage]
        at = lat.at[lat_rows(j, core, h, p)]
        remote(at, at, ag_s.at[d, stage, p], ag_r.at[d, stage, p], neighbour[d]).wait_recv()

    def forward(j, h, p):
        at = lat.at[lat_rows(j, core, h, p)]
        return remote(at, at, fw_s.at[j, h, p], fw_r.at[j, h, p], partner)

    def forward_wait(j):
        for h in range(2):
            for p in range(PIECES):
                at = lat.at[lat_rows(j, 1 - core, h, p)]
                remote(at, at, fw_s.at[j, h, p], fw_r.at[j, h, p], partner).wait_recv()

    lane = lax.broadcasted_iota(jnp.int32, (1, 128), 1)
    low = lax.rem(lane, ROPE) < ROPE // 2

    def turn(x, cosine, sine):
        swapped = jnp.where(low, pltpu.roll(x, 128 - ROPE // 2, 1), pltpu.roll(x, ROPE // 2, 1))
        return x * cosine + swapped * sine

    def up(j):
        at = chip_rows(j)
        cosine = tab[0, at, :]
        sine = tab[1, at, :]
        pair = 2 * (NOPE + ROPE)

        @pl.loop(0, 2)
        def _(i):
            start = pl.multiple_of(i * 2 * pair, 128)
            r = jnp.dot(lat[at, :q_width], wuq[:, pl.ds(start, 2 * pair)], preferred_element_type=F32)
            for k in range(2):
                x0 = r[:, k * pair : k * pair + 128]
                x1 = r[:, k * pair + 128 : k * pair + 256]
                x2 = r[:, k * pair + 256 : k * pair + 384]
                y1 = jnp.where(lane < ROPE, turn(x1, cosine, sine), x1)
                y2 = jnp.where(lane < ROPE, x2, turn(x2, cosine, sine))
                for n, y in enumerate((x0, y1, y2)):
                    to = pl.multiple_of(start + k * pair + n * 128, 128)
                    qbuf[at, pl.ds(to, 128)] = y.astype(BF16)

        @pl.loop(0, 4)
        def _(i):
            width = wukv.shape[1] // 4
            cols = pl.ds(pl.multiple_of(i * width, 128), width)
            r = jnp.dot(lat[at, q_width:], wukv[:, cols], preferred_element_type=F32)
            kvbuf[at, cols] = r.astype(BF16)

    def stores(j):
        at = chip_rows(j)
        return (
            pltpu.make_async_copy(qbuf.at[at], q_out.at[at], out_sem.at[2 * j]),
            pltpu.make_async_copy(kvbuf.at[at], kv_out.at[at], out_sem.at[2 * j + 1]),
        )

    hid_loads[opposite].wait()
    for copy in first_loads:
        copy.wait()
    for copy in late_loads:
        copy.start()
    down(opposite)
    pl.semaphore_wait(barrier, 3)
    pair_copies[opposite].start()
    hid_loads[1].wait()
    down(1)
    pair_copies[1].start()
    pair_copies[opposite].wait_recv()
    for p in range(PIECES):
        for d in range(2):
            ring_put(d, 0, p, chip_sum(opposite, d, p))
            ring_copy(d, 0, p).start()
    hid_loads[3].wait()
    down(3)
    pair_copies[3].start()
    pair_copies[1].wait_recv()
    for p in range(PIECES):
        ring_put(0, 1, p, chip_sum(1, 1, p))
        ring_copy(0, 1, p).start()
    hid_loads[0].wait()
    down(0)
    pair_copies[0].start()
    pair_copies[3].wait_recv()
    for p in range(PIECES):
        ring_put(1, 1, p, chip_sum(3, 0, p))
        ring_copy(1, 1, p).start()
    for copy in late_loads:
        copy.wait()

    for p in range(PIECES):
        for d in range(2):
            ring_copy(d, 0, p).wait_recv()
            ring_put(d, 2, p, chip_sum(toward[d], d, p) + ring_got(d, 0, p))
            ring_copy(d, 2, p).start()

    pair_copies[0].wait_recv()
    for p in range(PIECES):
        for h in range(2):
            ring_copy(1 - h, 1, p).wait_recv()
            ring_copy(h, 2, p).wait_recv()
            total = chip_sum(0, h, p) + ring_got(1 - h, 1, p) + ring_got(h, 2, p)
            q = total[:, :q_width]
            kv = total[:, q_width:latent_width]
            q_scale = lax.rsqrt(jnp.mean(q * q, axis=1, keepdims=True) + 1e-06)
            kv_scale = lax.rsqrt(jnp.mean(kv * kv, axis=1, keepdims=True) + 1e-06)
            at = lat_rows(0, core, h, p)
            lat[at, :q_width] = (q * q_scale * qg[...]).astype(BF16)
            lat[at, q_width:] = (kv * kv_scale * kvg[...]).astype(BF16)
            gather_copy(h, 0, p).start()
            gather_copy(1 - h, 1, p).start()
            forward(0, h, p).start()
            key = total[:, latent_width:]
            first = key[:, : ROPE // 2]
            second = key[:, ROPE // 2 :]
            cosine = tab[0, at, : ROPE // 2]
            sine = tab[1, at, ROPE // 2 : ROPE]
            keybuf[piece_rows(h, p), :] = jnp.concatenate(
                [first * cosine - second * sine, second * cosine + first * sine], axis=1
            ).astype(BF16)
    key_copy = pltpu.make_async_copy(keybuf, key_out, out_sem.at[8])
    key_copy.start()

    forward_wait(0)
    up(0)
    for copy in stores(0):
        copy.start()

    for p in range(PIECES):
        for d in range(2):
            gather_wait(d, 0, p)
            gather_copy(d, 2, p).start()
            forward(behind[d], d, p).start()
        for d in range(2):
            gather_wait(d, 1, p)
            forward(behind[d], 1 - d, p).start()
    for j in (1, 3):
        forward_wait(j)
        up(j)
        for copy in stores(j):
            copy.start()

    for p in range(PIECES):
        for d in range(2):
            gather_wait(d, 2, p)
            forward(opposite, d, p).start()
    forward_wait(opposite)
    up(opposite)
    for copy in stores(opposite):
        copy.start()

    for j in range(CHIPS):
        pair_copies[j].wait_send()
    for d in range(2):
        for stage in range(3):
            for p in range(PIECES):
                ring_copy(d, stage, p).wait_send()
                gather_copy(d, stage, p).wait_send()
    for j in range(CHIPS):
        for h in range(2):
            for p in range(PIECES):
                forward(j, h, p).wait_send()
    key_copy.wait()
    for j in range(CHIPS):
        for copy in stores(j):
            copy.wait()


def shards(hidden, w_dq, w_dkv, q_gain, kv_gain, w_uq, w_ukv):
    rows = hidden.shape[0]
    features, q_width = w_dq.shape
    kv_width = kv_gain.shape[0]
    down_width = q_width + w_dkv.shape[1]
    latent_width = q_width + kv_width
    block = rows // (2 * CHIPS)
    half = block // 2
    table = jnp.asarray(rotary_tables(rows))
    dma = pltpu.SemaphoreType.DMA
    any_spec = pl.BlockSpec(memory_space=pl.ANY)
    flops = 2 * rows * (features * down_width + q_width * w_uq.shape[1] + kv_width * w_ukv.shape[1])
    return pl.pallas_call(
        kernel,
        out_shape=(
            jax.ShapeDtypeStruct((rows, w_uq.shape[1]), BF16),
            jax.ShapeDtypeStruct((rows, w_ukv.shape[1]), BF16),
            jax.ShapeDtypeStruct((block, ROPE), BF16),
        ),
        in_specs=[any_spec] * 8,
        out_specs=(any_spec,) * 3,
        scratch_shapes=[
            pltpu.VMEM(hidden.shape, BF16),
            pltpu.VMEM(w_dq.shape, BF16),
            pltpu.VMEM(w_dkv.shape, BF16),
            pltpu.VMEM((1, q_width), F32),
            pltpu.VMEM((1, kv_width), F32),
            pltpu.VMEM(w_uq.shape, BF16),
            pltpu.VMEM(w_ukv.shape, BF16),
            pltpu.VMEM(table.shape, F32),
            pltpu.VMEM((CHIPS, block, down_width), F32),
            pltpu.VMEM((CHIPS, block, down_width), BF16),
            pltpu.VMEM((CHIPS, block, down_width), BF16),
            pltpu.VMEM((2, 3, half, down_width), BF16),
            pltpu.VMEM((2, 3, half, down_width), BF16),
            pltpu.VMEM((rows, latent_width), BF16),
            pltpu.VMEM((rows, w_uq.shape[1]), BF16),
            pltpu.VMEM((rows, w_ukv.shape[1]), BF16),
            pltpu.VMEM((block, ROPE), BF16),
            dma((11,)),
            dma((CHIPS,)), dma((CHIPS,)),
            dma((2, 3, PIECES)), dma((2, 3, PIECES)),
            dma((2, 3, PIECES)), dma((2, 3, PIECES)),
            dma((CHIPS, 2, PIECES)), dma((CHIPS, 2, PIECES)),
            dma((9,)),
        ],
        compiler_params=pltpu.CompilerParams(
            collective_id=0, has_side_effects=True, vmem_limit_bytes=60 * 1024 * 1024
        ),
        cost_estimate=pl.CostEstimate(flops=flops, bytes_accessed=20_000_000, transcendentals=0),
    )(
        hidden, w_dq, w_dkv, q_gain.reshape(1, -1), kv_gain.reshape(1, -1), w_uq, w_ukv, table
    )


def solution(mesh):
    in_specs = (
        P("dp", "tensor"),
        P("tensor", None),
        P("tensor", None),
        P(),
        P(),
        P(None, "tensor"),
        P(None, "tensor"),
    )
    out_specs = (P("dp", "tensor"), P("dp", "tensor"), P(("dp", "tensor"), None))
    return jax.shard_map(shards, mesh=mesh, in_specs=in_specs, out_specs=out_specs, check_vma=False)
```

```python
import jax
import jax.numpy as jnp
import numpy as np
from jax import lax
from jax.experimental import pallas as pl
from jax.experimental.pallas import tpu as pltpu
from jax.sharding import PartitionSpec as P

NOPE = 128
ROPE = 64
CHIPS = 4
PIECES = 4
WINDOW = 3
TILE = 16
LANES = 128
MESH = pl.DeviceIdType.MESH
F32 = jnp.float32
BF16 = jnp.bfloat16


def rotary_tables(count):
    half = ROPE // 2
    freqs = (50000.0 ** (-np.arange(half, dtype=np.float32) / half)).astype(np.float32)
    angle = np.arange(count, dtype=np.float32)[:, None] * freqs[None, :]
    cosine = np.cos(angle.astype(np.float64)).astype(np.float32)
    sine = np.sin(angle.astype(np.float64)).astype(np.float32)
    cosine = np.tile(cosine, (1, 4))
    sine = np.concatenate([-sine, sine, -sine, sine], axis=1)
    return np.stack([cosine, sine])


def lanes():
    return lax.broadcasted_iota(jnp.int32, (1, LANES), 1)


def turn(x, cosine, sine):
    low = lax.rem(lanes(), ROPE) < ROPE // 2
    swapped = jnp.where(low, pltpu.roll(x, LANES - ROPE // 2, 1), pltpu.roll(x, ROPE // 2, 1))
    return x * cosine + swapped * sine


def up_queries(blocks, lat, wuq, tab, put):
    q_width = wuq.shape[0]
    pair = 2 * (NOPE + ROPE)
    steps = wuq.shape[1] // (2 * pair)
    lane = lanes()

    @pl.loop(0, steps)
    def _(i):
        start = pl.multiple_of(i * 2 * pair, LANES)
        x = jnp.concatenate([lat[at, :q_width] for at in blocks], axis=0)
        cosine = jnp.concatenate([tab[0, at, :] for at in blocks], axis=0)
        sine = jnp.concatenate([tab[1, at, :] for at in blocks], axis=0)
        r = jnp.dot(x, wuq[:, pl.ds(start, 2 * pair)], preferred_element_type=F32)
        for k in range(2):
            x0 = r[:, k * pair : k * pair + 128]
            x1 = r[:, k * pair + 128 : k * pair + 256]
            x2 = r[:, k * pair + 256 : k * pair + 384]
            y1 = jnp.where(lane < ROPE, turn(x1, cosine, sine), x1)
            y2 = jnp.where(lane < ROPE, x2, turn(x2, cosine, sine))
            for n, y in enumerate((x0, y1, y2)):
                y = y.astype(BF16)
                row = 0
                for b, at in enumerate(blocks):
                    put(b, pl.multiple_of(start + k * pair + n * LANES, LANES), y[row : row + at.size])
                    row += at.size


def up_keys_values(blocks, lat, wukv, put):
    q_width = lat.shape[1] - wukv.shape[0]
    width = 512

    @pl.loop(0, wukv.shape[1] // width)
    def _(i):
        start = pl.multiple_of(i * width, LANES)
        x = jnp.concatenate([lat[at, q_width:] for at in blocks], axis=0)
        y = jnp.dot(x, wukv[:, pl.ds(start, width)], preferred_element_type=F32).astype(BF16)
        row = 0
        for b, at in enumerate(blocks):
            put(b, start, y[row : row + at.size])
            row += at.size


def place():
    me = lax.axis_index("tensor")
    chip = me // 2
    core = me - 2 * chip
    return me, chip, core


def quarter_blocks(chip, block, offsets, g):
    size = block // 4
    return [
        pl.ds(pl.multiple_of((lax.rem(chip + j, CHIPS) * 2 + c) * block + h * 2 * size + g * size, size), size)
        for j in offsets for c in range(2) for h in range(2)
    ]


def kernel(
    hidden, w_dq, w_dkv, q_gain, kv_gain, w_uq, w_ukv, table,
    qbuf, kvbuf, keybuf, lat, wuq, wukv, tab,
    hid, wdq, wdkv, gain, acc, pair_out, pair_in, ring_out, ring_in, keyrow,
    load_sem, first_s, first_r, pair_s, pair_r, rs_s, rs_r, ag_s, ag_r, fw_s, fw_r,
):
    rows = hid.shape[0]
    q_width = w_uq.shape[0]
    kv_width = w_ukv.shape[0]
    latent_width = q_width + kv_width
    q_tiles, tiles = q_width // LANES, latent_width // LANES
    block = rows // (2 * CHIPS)
    half = block // 2
    row_tiles = block // TILE
    strips = 4
    wide = tiles // strips
    me, chip, core = place()
    partner = me + 1 - 2 * core

    def chip_at(j):
        return lax.rem(chip + j, CHIPS)

    neighbour = (chip_at(1) * 2 + core, chip_at(CHIPS - 1) * 2 + core)
    toward = (1, CHIPS - 1)
    behind = (CHIPS - 1, 1)
    opposite = 2

    def load(i, src, dst):
        return pltpu.make_async_copy(src, dst, load_sem.at[i])

    def chip_rows(j):
        return pl.ds(pl.multiple_of(chip_at(j) * 2 * block, 2 * block), 2 * block)

    width = wide * LANES
    hid_loads = [load(j, hidden.at[chip_rows(j)], hid.at[chip_rows(j)]) for j in range(CHIPS)]
    strip_loads = [load(4 + i, w_dq.at[:, pl.ds(i * width, width)], wdq.at[i]) for i in range(strips - 1)]
    strip_loads.append(load(7, w_dkv, wdkv.at[pl.ds(0, kv_width + ROPE)]))
    late_loads = [
        load(8, q_gain, gain.at[pl.ds(0, q_tiles)]), load(9, kv_gain, gain.at[pl.ds(q_tiles, tiles - q_tiles)]),
        load(10, table, tab), load(11, w_ukv, wukv), load(12, w_uq, wuq),
    ]
    hid_loads[opposite].start()
    for copy in strip_loads:
        copy.start()
    for j in (1, 3, 0):
        hid_loads[j].start()

    barrier = pltpu.get_barrier_semaphore()
    for device in (*neighbour, partner):
        pl.semaphore_signal(barrier, inc=1, device_id={"tensor": device}, device_id_type=MESH)
    wdkv[kv_width + ROPE :, :] = jnp.zeros((ROPE, wdkv.shape[1]), BF16)

    def remote(src, dst, send, recv, device):
        return pltpu.make_async_remote_copy(
            src_ref=src, dst_ref=dst, send_sem=send, recv_sem=recv,
            device_id={"tensor": device}, device_id_type=MESH,
        )

    rotary_at = strips * row_tiles * wide
    lane = lanes()

    def down_strip(j, i, weights, depth):
        base = chip_at(j) * 2 * block
        other = pl.ds(pl.multiple_of(base + (1 - core) * block, block), block)
        own = pl.ds(pl.multiple_of(base + core * block, block), block)
        x = jnp.concatenate([hid[other, :], hid[own, :]], axis=0)
        r = lax.dot_general(x, weights, (((1,), (depth,)), ((), ())), preferred_element_type=F32)
        first = i * row_tiles * wide
        for t in range(row_tiles):
            for c in range(wide):
                cols = slice(c * LANES, (c + 1) * LANES)
                low = t * TILE
                pair_out[j, first + t * wide + c] = r[low : low + TILE, cols].astype(BF16)
                acc[j, first + t * wide + c] = r[block + low : block + low + TILE, cols]

    def down_rotary(j):
        base = chip_at(j) * 2 * block
        other = pl.ds(pl.multiple_of(base + (1 - core) * block, block), block)
        own = pl.ds(pl.multiple_of(base + core * block, block), block)
        x = jnp.concatenate([hid[other, :], hid[own, :]], axis=0)
        r = lax.dot_general(x, wdkv[kv_width:, :], (((1,), (1,)), ((), ())), preferred_element_type=F32)
        for side in range(2):
            for g in range(row_tiles // 2):
                low = side * block + g * 2 * TILE
                a, b = r[low : low + TILE], r[low + TILE : low + 2 * TILE]
                packed = jnp.where(lane < ROPE, a, pltpu.roll(b, ROPE, 1))
                if side == 0:
                    pair_out[j, rotary_at + g] = packed.astype(BF16)
                else:
                    acc[j, rotary_at + g] = packed

    def down_last(j):
        down_strip(j, strips - 1, wdkv[:kv_width, :], 1)
        down_rotary(j)

    def first_copy(i):
        size = row_tiles * wide
        at = pl.ds(i * size, size + (row_tiles // 2 if i == strips - 1 else 0))
        return remote(
            pair_out.at[opposite, at], pair_in.at[opposite, at], first_s.at[i], first_r.at[i], partner
        )

    def pair_copy(j):
        return remote(pair_out.at[j], pair_in.at[j], pair_s.at[j], pair_r.at[j], partner)

    def strip_sum(j, i, t, count):
        at = pl.ds((i * row_tiles + t) * wide, count * wide)
        return acc[j, at] + pair_in[j, at].astype(F32)

    def row_sum(j, t):
        return jnp.concatenate([strip_sum(j, i, t, 1) for i in range(strips)], axis=0)

    def rotary_sum(j, h):
        at = pl.ds(rotary_at + h * 2, 2)
        return acc[j, at] + pair_in[j, at].astype(F32)

    def run(stage, p):
        if stage == 0:
            return pl.ds(p * tiles, tiles + (2 if p == PIECES - 1 else 0))
        return pl.ds(0, tiles + 2) if p == 0 else pl.ds(p * tiles + 2, tiles)

    def run_tiles(stage, p):
        return pl.ds(run(stage, p).start, tiles)

    def rotary_tiles(stage):
        return pl.ds(PIECES * tiles if stage == 0 else tiles, 2)

    def ring_copy(d, stage, p):
        at = run(stage, p)
        return remote(
            ring_out.at[d, stage, at], ring_in.at[d, stage, at],
            rs_s.at[d, stage, p], rs_r.at[d, stage, p], neighbour[d],
        )

    def lat_rows(j, c, h, p):
        start = (chip_at(j) * 2 + c) * block + h * half + p * TILE
        return pl.ds(pl.multiple_of(start, TILE), TILE)

    def gather_copy(d, stage, p):
        j = (0, 0, behind[d])[stage]
        h = (d, 1 - d, d)[stage]
        at = lat.at[lat_rows(j, core, h, p)]
        return remote(at, at, ag_s.at[d, stage, p], ag_r.at[d, stage, p], neighbour[d])

    def gather_wait(d, stage, p):
        j = (behind[d], behind[d], opposite)[stage]
        h = (d, 1 - d, d)[stage]
        at = lat.at[lat_rows(j, core, h, p)]
        remote(at, at, ag_s.at[d, stage, p], ag_r.at[d, stage, p], neighbour[d]).wait_recv()

    def forward(j, h, p):
        at = lat.at[lat_rows(j, core, h, p)]
        return remote(at, at, fw_s.at[j, h, p], fw_r.at[j, h, p], partner)

    def forward_wait(j, p):
        for h in range(2):
            at = lat.at[lat_rows(j, 1 - core, h, p)]
            remote(at, at, fw_s.at[j, h, p], fw_r.at[j, h, p], partner).wait_recv()

    sent = ([], [])

    def send(d, copy):
        if len(sent[d]) >= PIECES:
            sent[d][len(sent[d]) - WINDOW].wait_send()
        copy.start()
        sent[d].append(copy)

    def queries_in(blocks):
        def put(b, column, values):
            qbuf[blocks[b], pl.ds(column, LANES)] = values
        up_queries(blocks, lat, wuq, tab, put)

    def keys_values_in(blocks):
        def put(b, column, values):
            kvbuf[blocks[b], pl.ds(column, 512)] = values
        up_keys_values(blocks, lat, wukv, put)

    def first_send(i):
        first_copy(i).wait_recv()
        for d in range(2):
            t = d * PIECES
            ring_out[d, 0, pl.ds(i * tiles, tiles)] = strip_sum(opposite, i, t, PIECES).astype(BF16)
            if i == strips - 1:
                ring_out[d, 0, rotary_tiles(0)] = rotary_sum(opposite, d).astype(BF16)
            send(d, ring_copy(d, 0, i))

    hid_loads[opposite].wait()
    for i in range(strips):
        strip_loads[i].wait()
        if i < strips - 1:
            down_strip(opposite, i, wdq[i], 0)
        else:
            down_last(opposite)
        if i == 0:
            pl.semaphore_wait(barrier, 3)
        first_copy(i).start()
        if i == 1:
            for copy in late_loads:
                copy.start()
        if i > 0:
            first_send(i - 1)
    first_send(strips - 1)

    for j in (1, 3, 0):
        hid_loads[j].wait()

        @pl.loop(0, strips - 1)
        def _(i):
            down_strip(j, i, wdq[i], 0)

        down_last(j)
        pair_copy(j).start()

    for copy in late_loads:
        copy.wait()

    for d in range(2):
        pair_copy(toward[d]).wait_recv()
    for p in range(PIECES):
        for d in range(2):
            h = 1 - d
            ring_out[d, 1, run_tiles(1, p)] = row_sum(toward[d], h * PIECES + p).astype(BF16)
            if p == 0:
                ring_out[d, 1, rotary_tiles(1)] = rotary_sum(toward[d], h).astype(BF16)
            send(d, ring_copy(d, 1, p))

    for i in range(strips):
        for d in range(2):
            ring_copy(d, 0, i).wait_recv()
    for p in range(PIECES):
        for d in range(2):
            got = jnp.concatenate(
                [ring_in[d, 0, pl.ds(i * tiles + p * wide, wide)] for i in range(strips)], axis=0
            ).astype(F32)
            total = row_sum(toward[d], d * PIECES + p) + got
            ring_out[d, 2, run_tiles(2, p)] = total.astype(BF16)
            if p == 0:
                total = rotary_sum(toward[d], d) + ring_in[d, 0, rotary_tiles(0)].astype(F32)
                ring_out[d, 2, rotary_tiles(2)] = total.astype(BF16)
            send(d, ring_copy(d, 2, p))

    pair_copy(0).wait_recv()
    for p in range(PIECES):
        for h in range(2):
            ring_copy(1 - h, 1, p).wait_recv()
            ring_copy(h, 2, p).wait_recv()
            total = row_sum(0, h * PIECES + p)
            total += ring_in[1 - h, 1, run_tiles(1, p)].astype(F32) + ring_in[h, 2, run_tiles(2, p)].astype(F32)
            at = lat_rows(0, core, h, p)
            for first, end in ((0, q_tiles), (q_tiles, tiles)):
                part = total[first:end]
                squares = jnp.sum(jnp.sum(part * part, axis=0), axis=1, keepdims=True)
                scale = lax.rsqrt(squares / ((end - first) * LANES) + 1e-06)
                for k in range(first, end):
                    value = total[k] * scale * gain[k : k + 1, :]
                    lat[at, k * LANES : (k + 1) * LANES] = value.astype(BF16)
            forward(0, h, p).start()
        for d in range(2):
            send(d, gather_copy(d, 0, p))
        for d in range(2):
            send(d, gather_copy(d, 1, p))
    for h in range(2):
        total = rotary_sum(0, h)
        total += ring_in[1 - h, 1, rotary_tiles(1)].astype(F32) + ring_in[h, 2, rotary_tiles(2)].astype(F32)
        for g in range(2):
            a, b = lat_rows(0, core, h, 2 * g), lat_rows(0, core, h, 2 * g + 1)
            cosine = jnp.where(lane < ROPE, tab[0, a, :], tab[0, b, :])
            sine = jnp.where(lane < ROPE, tab[1, a, :], tab[1, b, :])
            turned = turn(total[g], cosine, sine)
            low = h * half + 2 * g * TILE
            keyrow[low : low + TILE, :] = turned
            keyrow[low + TILE : low + 2 * TILE, :] = pltpu.roll(turned, ROPE, 1)
    keybuf[...] = keyrow[...].T[:ROPE].astype(BF16)

    for p in range(PIECES):
        forward_wait(0, p)
    queries_in([chip_rows(0)])

    for p in range(PIECES):
        for d in range(2):
            gather_wait(d, 0, p)
            forward(behind[d], d, p).start()
            send(d, gather_copy(d, 2, p))
        if p == 0:
            keys_values_in([chip_rows(0)])
        for d in range(2):
            gather_wait(d, 1, p)
            forward(behind[d], 1 - d, p).start()
        if p == 1:
            near = quarter_blocks(chip, block, (1, 3), 0)
            for q in range(2):
                forward_wait(1, q)
                forward_wait(3, q)
            queries_in(near)
    keys_values_in(near)
    near = quarter_blocks(chip, block, (1, 3), 1)
    for q in range(2, PIECES):
        forward_wait(1, q)
        forward_wait(3, q)
    queries_in(near)

    for p in range(PIECES // 2):
        for d in range(2):
            gather_wait(d, 2, p)
            forward(opposite, d, p).start()
    keys_values_in(near)
    for p in range(PIECES // 2):
        forward_wait(opposite, p)
    far = quarter_blocks(chip, block, (opposite,), 0)
    queries_in(far)
    keys_values_in(far)
    for p in range(PIECES // 2, PIECES):
        for d in range(2):
            gather_wait(d, 2, p)
            forward(opposite, d, p).start()

    for i in range(strips):
        first_copy(i).wait_send()
    for j in (1, 3, 0):
        pair_copy(j).wait_send()
    for d in range(2):
        for copy in sent[d][: PIECES - WINDOW] + sent[d][len(sent[d]) - WINDOW :]:
            copy.wait_send()
    for j in range(CHIPS):
        for h in range(2):
            for p in range(PIECES):
                forward(j, h, p).wait_send()
    for p in range(PIECES // 2, PIECES):
        forward_wait(opposite, p)


def store(q, kv, key, lat, wuq, wukv, tab, q_out, kv_out, key_out, qlast, kvlast, sem, last_sem):
    _, chip, _ = place()
    block = q.shape[0] // (2 * CHIPS)
    last = quarter_blocks(chip, block, (2,), 1)
    copies = [pltpu.make_async_copy(key, key_out, sem.at[0])]

    def add(at):
        for src, dst in ((q, q_out), (kv, kv_out)):
            copies.append(pltpu.make_async_copy(src.at[at], dst.at[at], sem.at[len(copies)]))

    for j in (0, 1, 3):
        add(pl.ds(pl.multiple_of(lax.rem(chip + j, CHIPS) * 2 * block, 2 * block), 2 * block))
    for at in quarter_blocks(chip, block, (2,), 0):
        add(at)
    for copy in copies:
        copy.start()

    def put_q(b, column, values):
        qlast[b * (block // 4) : (b + 1) * (block // 4), pl.ds(column, LANES)] = values

    def put_kv(b, column, values):
        kvlast[b * (block // 4) : (b + 1) * (block // 4), pl.ds(column, 512)] = values

    def finish(n, src, dst):
        made = [
            pltpu.make_async_copy(src.at[pl.ds(b * (block // 4), block // 4)], dst.at[at], last_sem.at[n, b])
            for b, at in enumerate(last)
        ]
        for copy in made:
            copy.start()
        copies.extend(made)

    up_keys_values(last, lat, wukv, put_kv)
    finish(0, kvlast, kv_out)
    up_queries(last, lat, wuq, tab, put_q)
    finish(1, qlast, q_out)
    for copy in copies:
        copy.wait()


def shards(hidden, w_dq, w_dkv, q_gain, kv_gain, w_uq, w_ukv):
    rows = hidden.shape[0]
    features, q_width = w_dq.shape
    w_dkv = w_dkv.T
    kv_width = kv_gain.shape[0]
    tiles = (q_width + kv_width) // LANES
    block = rows // (2 * CHIPS)
    table = jnp.asarray(rotary_tables(rows))
    dma = pltpu.SemaphoreType.DMA
    any_spec = pl.BlockSpec(memory_space=pl.ANY)
    vmem_spec = pl.BlockSpec(memory_space=pltpu.VMEM)
    shapes = ((rows, w_uq.shape[1]), (rows, w_ukv.shape[1]), (ROPE, block))
    flops = 2 * rows * (features * (q_width + w_dkv.shape[0]) + q_width * w_uq.shape[1] + kv_width * w_ukv.shape[1])
    pair_tiles = (block // TILE) * tiles + block // TILE // 2
    results = pl.pallas_call(
        kernel,
        out_shape=(
            *(pltpu.VMEM(shape, BF16) for shape in shapes),
            pltpu.VMEM((rows, q_width + kv_width), BF16),
            pltpu.VMEM(w_uq.shape, BF16),
            pltpu.VMEM(w_ukv.shape, BF16),
            pltpu.VMEM(table.shape, F32),
        ),
        in_specs=[any_spec] * 8,
        out_specs=(vmem_spec,) * 7,
        scratch_shapes=[
            pltpu.VMEM(hidden.shape, BF16),
            pltpu.VMEM((3, features, q_width // 3), BF16),
            pltpu.VMEM((kv_width + 2 * ROPE, features), BF16),
            pltpu.VMEM((tiles, LANES), F32),
            pltpu.VMEM((CHIPS, pair_tiles, TILE, LANES), F32),
            pltpu.VMEM((CHIPS, pair_tiles, TILE, LANES), BF16),
            pltpu.VMEM((CHIPS, pair_tiles, TILE, LANES), BF16),
            pltpu.VMEM((2, 3, PIECES * tiles + 2, TILE, LANES), BF16),
            pltpu.VMEM((2, 3, PIECES * tiles + 2, TILE, LANES), BF16),
            pltpu.VMEM((block, LANES), F32),
            dma((13,)),
            dma((4,)), dma((4,)),
            dma((CHIPS,)), dma((CHIPS,)),
            dma((2, 3, PIECES)), dma((2, 3, PIECES)),
            dma((2, 3, PIECES)), dma((2, 3, PIECES)),
            dma((CHIPS, 2, PIECES)), dma((CHIPS, 2, PIECES)),
        ],
        compiler_params=pltpu.CompilerParams(
            collective_id=0, has_side_effects=True, vmem_limit_bytes=47_000_000
        ),
        cost_estimate=pl.CostEstimate(flops=flops, bytes_accessed=13_000_000, transcendentals=0),
    )(
        hidden, w_dq, w_dkv, q_gain.reshape(-1, LANES), kv_gain.reshape(-1, LANES), w_uq, w_ukv, table
    )
    queries, keys_values, rotary = pl.pallas_call(
        store,
        out_shape=tuple(jax.ShapeDtypeStruct(shape, BF16) for shape in shapes),
        in_specs=[vmem_spec] * 7,
        out_specs=(any_spec,) * 3,
        scratch_shapes=[
            pltpu.VMEM((block, w_uq.shape[1]), BF16),
            pltpu.VMEM((block, w_ukv.shape[1]), BF16),
            dma((15,)),
            dma((2, 4)),
        ],
        compiler_params=pltpu.CompilerParams(vmem_limit_bytes=8 * 1024 * 1024),
        cost_estimate=pl.CostEstimate(flops=flops // 16, bytes_accessed=7_400_000, transcendentals=0),
    )(*results)
    return queries, keys_values, rotary.T


def solution(mesh):
    in_specs = (
        P("dp", "tensor"),
        P("tensor", None),
        P("tensor", None),
        P(),
        P(),
        P(None, "tensor"),
        P(None, "tensor"),
    )
    out_specs = (P("dp", "tensor"), P("dp", "tensor"), P(("dp", "tensor"), None))
    return jax.shard_map(shards, mesh=mesh, in_specs=in_specs, out_specs=out_specs, check_vma=False)
```

```python
import jax
import jax.numpy as jnp
import numpy as np
from jax import lax
from jax.experimental import pallas as pl
from jax.experimental.pallas import tpu as pltpu
from jax.sharding import PartitionSpec as P

NOPE = 128
ROPE = 64
CHIPS = 4
PIECES = 4
WINDOW = 3
TILE = 16
LANES = 128
MESH = pl.DeviceIdType.MESH
F32 = jnp.float32
BF16 = jnp.bfloat16


def rotary_tables(count):
    half = ROPE // 2
    freqs = (50000.0 ** (-np.arange(half, dtype=np.float32) / half)).astype(np.float32)
    angle = np.arange(count, dtype=np.float32)[:, None] * freqs[None, :]
    cosine = np.cos(angle.astype(np.float64)).astype(np.float32)
    sine = np.sin(angle.astype(np.float64)).astype(np.float32)
    cosine = np.tile(cosine, (1, 4))
    sine = np.concatenate([-sine, sine, -sine, sine], axis=1)
    return np.stack([cosine, sine])


def lanes():
    return lax.broadcasted_iota(jnp.int32, (1, LANES), 1)


def turn(x, cosine, sine):
    low = lax.rem(lanes(), ROPE) < ROPE // 2
    swapped = jnp.where(low, pltpu.roll(x, LANES - ROPE // 2, 1), pltpu.roll(x, ROPE // 2, 1))
    return x * cosine + swapped * sine


def up_queries(blocks, lat, wuq, tab, put, steps):
    q_width = wuq.shape[0]
    pair = 2 * (NOPE + ROPE)
    heads = wuq.shape[1] // (steps * pair)
    lane = lanes()

    @pl.loop(0, steps)
    def _(i):
        start = pl.multiple_of(i * heads * pair, LANES)
        x = jnp.concatenate([lat[at, :q_width] for at in blocks], axis=0)
        cosine = jnp.concatenate([tab[0, at, :] for at in blocks], axis=0)
        sine = jnp.concatenate([tab[1, at, :] for at in blocks], axis=0)
        r = jnp.dot(x, wuq[:, pl.ds(start, heads * pair)], preferred_element_type=F32)
        for k in range(heads):
            x0 = r[:, k * pair : k * pair + 128]
            x1 = r[:, k * pair + 128 : k * pair + 256]
            x2 = r[:, k * pair + 256 : k * pair + 384]
            y1 = jnp.where(lane < ROPE, turn(x1, cosine, sine), x1)
            y2 = jnp.where(lane < ROPE, x2, turn(x2, cosine, sine))
            for n, y in enumerate((x0, y1, y2)):
                y = y.astype(BF16)
                row = 0
                for b, at in enumerate(blocks):
                    put(b, pl.multiple_of(start + k * pair + n * LANES, LANES), y[row : row + at.size])
                    row += at.size


def up_keys_values(blocks, lat, wukv, put, steps):
    q_width = lat.shape[1] - wukv.shape[0]
    width = wukv.shape[1] // steps

    @pl.loop(0, steps)
    def _(i):
        start = pl.multiple_of(i * width, LANES)
        x = jnp.concatenate([lat[at, q_width:] for at in blocks], axis=0)
        y = jnp.dot(x, wukv[:, pl.ds(start, width)], preferred_element_type=F32).astype(BF16)
        row = 0
        for b, at in enumerate(blocks):
            put(b, start, y[row : row + at.size])
            row += at.size


def place():
    me = lax.axis_index("tensor")
    chip = me // 2
    core = me - 2 * chip
    return me, chip, core


def piece_blocks(chip, block, offsets, first, count):
    size = count * TILE
    return [
        pl.ds(pl.multiple_of((lax.rem(chip + j, CHIPS) * 2 + c) * block + h * (block // 2) + first * TILE, TILE), size)
        for j in offsets for c in range(2) for h in range(2)
    ]


def kernel(
    hidden, w_dq, w_dkv, q_gain, kv_gain, w_uq, w_ukv, table,
    qbuf, kvbuf, keybuf, lat, wuq, wukv, tab,
    hid, wdq, wdkv, gain, acc, pair_out, pair_in, ring_out, ring_in, keyrow,
    load_sem, first_r, pair_s, pair_r, ring_s, rs_first_r, rs_r, ag_r, fw_s, fw_r,
):
    rows = hid.shape[0]
    q_width = w_uq.shape[0]
    kv_width = w_ukv.shape[0]
    latent_width = q_width + kv_width
    q_tiles, tiles = q_width // LANES, latent_width // LANES
    block = rows // (2 * CHIPS)
    half = block // 2
    row_tiles = block // TILE
    strips = 4
    wide = tiles // strips
    me, chip, core = place()
    partner = me + 1 - 2 * core

    def chip_at(j):
        return lax.rem(chip + j, CHIPS)

    neighbour = (chip_at(1) * 2 + core, chip_at(CHIPS - 1) * 2 + core)
    toward = (1, CHIPS - 1)
    behind = (CHIPS - 1, 1)
    opposite = 2

    def load(i, src, dst):
        return pltpu.make_async_copy(src, dst, load_sem.at[i])

    def chip_rows(j):
        return pl.ds(pl.multiple_of(chip_at(j) * 2 * block, 2 * block), 2 * block)

    width = wide * LANES
    hid_loads = [load(j, hidden.at[chip_rows(j)], hid.at[chip_rows(j)]) for j in range(CHIPS)]
    strip_loads = [load(4 + i, w_dq.at[:, pl.ds(i * width, width)], wdq.at[i]) for i in range(strips - 1)]
    strip_loads.append(load(7, w_dkv, wdkv.at[pl.ds(0, kv_width + ROPE)]))
    late_loads = [
        load(8, q_gain, gain.at[pl.ds(0, q_tiles)]), load(9, kv_gain, gain.at[pl.ds(q_tiles, tiles - q_tiles)]),
        load(10, table, tab), load(11, w_ukv, wukv), load(12, w_uq, wuq),
    ]
    hid_loads[opposite].start()
    for copy in strip_loads:
        copy.start()
    for j in (1, 3, 0):
        hid_loads[j].start()

    barrier = pltpu.get_barrier_semaphore()
    for device in (*neighbour, partner):
        pl.semaphore_signal(barrier, inc=1, device_id={"tensor": device}, device_id_type=MESH)
    wdkv[kv_width + ROPE :, :] = jnp.zeros((ROPE, wdkv.shape[1]), BF16)

    def remote(src, dst, send, recv, device):
        return pltpu.make_async_remote_copy(
            src_ref=src, dst_ref=dst, send_sem=send, recv_sem=recv,
            device_id={"tensor": device}, device_id_type=MESH,
        )

    rotary_at = strips * row_tiles * wide
    lane = lanes()

    def down_strip(j, i, weights, depth):
        base = chip_at(j) * 2 * block
        other = pl.ds(pl.multiple_of(base + (1 - core) * block, block), block)
        own = pl.ds(pl.multiple_of(base + core * block, block), block)
        x = jnp.concatenate([hid[other, :], hid[own, :]], axis=0)
        r = lax.dot_general(x, weights, (((1,), (depth,)), ((), ())), preferred_element_type=F32)
        first = i * row_tiles * wide
        for t in range(row_tiles):
            for c in range(wide):
                cols = slice(c * LANES, (c + 1) * LANES)
                low = t * TILE
                pair_out[j, first + t * wide + c] = r[low : low + TILE, cols].astype(BF16)
                acc[j, first + t * wide + c] = r[block + low : block + low + TILE, cols]

    def down_rotary(j):
        base = chip_at(j) * 2 * block
        other = pl.ds(pl.multiple_of(base + (1 - core) * block, block), block)
        own = pl.ds(pl.multiple_of(base + core * block, block), block)
        x = jnp.concatenate([hid[other, :], hid[own, :]], axis=0)
        r = lax.dot_general(x, wdkv[kv_width:, :], (((1,), (1,)), ((), ())), preferred_element_type=F32)
        for side in range(2):
            for g in range(row_tiles // 2):
                low = side * block + g * 2 * TILE
                a, b = r[low : low + TILE], r[low + TILE : low + 2 * TILE]
                packed = jnp.where(lane < ROPE, a, pltpu.roll(b, ROPE, 1))
                if side == 0:
                    pair_out[j, rotary_at + g] = packed.astype(BF16)
                else:
                    acc[j, rotary_at + g] = packed

    def down_last(j):
        down_strip(j, strips - 1, wdkv[:kv_width, :], 1)
        down_rotary(j)

    def first_copy(i):
        size = row_tiles * wide
        at = pl.ds(i * size, size + (row_tiles // 2 if i == strips - 1 else 0))
        return remote(
            pair_out.at[opposite, at], pair_in.at[opposite, at], pair_s.at[0], first_r.at[i], partner
        )

    def pair_copy(j):
        return remote(pair_out.at[j], pair_in.at[j], pair_s.at[0], pair_r.at[j], partner)

    def strip_sum(j, i, t, count):
        at = pl.ds((i * row_tiles + t) * wide, count * wide)
        return acc[j, at] + pair_in[j, at].astype(F32)

    def row_sum(j, t):
        return jnp.concatenate([strip_sum(j, i, t, 1) for i in range(strips)], axis=0)

    def rotary_sum(j, h):
        at = pl.ds(rotary_at + h * 2, 2)
        return acc[j, at] + pair_in[j, at].astype(F32)

    def run(stage, p):
        if stage == 0:
            return pl.ds(p * tiles, tiles + (2 if p == PIECES - 1 else 0))
        return pl.ds(0, tiles + 2) if p == 0 else pl.ds(p * tiles + 2, tiles)

    def run_tiles(stage, p):
        return pl.ds(run(stage, p).start, tiles)

    def rotary_tiles(stage):
        return pl.ds(PIECES * tiles if stage == 0 else tiles, 2)

    def ring_copy(d, stage, p, n=0):
        at = run(stage, p)
        recv = rs_first_r.at[d] if stage == 0 else rs_r.at[d, stage - 1, p]
        return remote(
            ring_out.at[d, stage, at], ring_in.at[d, stage, at], ring_s.at[d, n % PIECES], recv, neighbour[d]
        )

    def ring_first_wait(d):
        remote(
            ring_out.at[d, 0], ring_in.at[d, 0], ring_s.at[d, 0], rs_first_r.at[d], neighbour[d]
        ).wait_recv()

    def lat_rows(j, c, h, p):
        start = (chip_at(j) * 2 + c) * block + h * half + p * TILE
        return pl.ds(pl.multiple_of(start, TILE), TILE)

    def gather_copy(d, stage, p, n):
        j = (0, 0, behind[d])[stage]
        h = (d, 1 - d, d)[stage]
        at = lat.at[lat_rows(j, core, h, p)]
        return remote(at, at, ring_s.at[d, n % PIECES], ag_r.at[d, stage, p], neighbour[d])

    def gather_wait(d, stage, p):
        j = (behind[d], behind[d], opposite)[stage]
        h = (d, 1 - d, d)[stage]
        at = lat.at[lat_rows(j, core, h, p)]
        remote(at, at, ring_s.at[d, 0], ag_r.at[d, stage, p], neighbour[d]).wait_recv()

    def forward(j, h, p):
        at = lat.at[lat_rows(j, core, h, p)]
        return remote(at, at, fw_s.at[0], fw_r.at[j, p], partner)

    def forward_wait(j, p):
        at = lat.at[pl.ds(0, 2 * TILE)]
        remote(at, at, fw_s.at[0], fw_r.at[j, p], partner).wait_recv()

    sent = ([], [])

    done = [0, 0]

    def drain(d, end):
        for copy in sent[d][done[d] : end]:
            copy.wait_send()
        done[d] = end

    def send(d, make, *which):
        n = len(sent[d])
        if n >= PIECES:
            drain(d, n - WINDOW + 1)
        copy = make(d, *which, n)
        copy.start()
        sent[d].append(copy)

    def queries_in(blocks):
        def put(b, column, values):
            qbuf[blocks[b], pl.ds(column, LANES)] = values
        up_queries(blocks, lat, wuq, tab, put, 1)

    def keys_values_in(blocks):
        def put(b, column, values):
            kvbuf[blocks[b], pl.ds(column, values.shape[1])] = values
        up_keys_values(blocks, lat, wukv, put, 1)

    def first_send(i):
        first_copy(i).wait_recv()
        for d in range(2):
            t = d * PIECES
            ring_out[d, 0, pl.ds(i * tiles, tiles)] = strip_sum(opposite, i, t, PIECES).astype(BF16)
            if i == strips - 1:
                ring_out[d, 0, rotary_tiles(0)] = rotary_sum(opposite, d).astype(BF16)
            send(d, ring_copy, 0, i)

    hid_loads[opposite].wait()
    for i in range(strips):
        strip_loads[i].wait()
        if i < strips - 1:
            down_strip(opposite, i, wdq[i], 0)
        else:
            down_last(opposite)
        if i == 0:
            pl.semaphore_wait(barrier, 3)
        first_copy(i).start()
        if i == 1:
            for copy in late_loads:
                copy.start()
        if i > 0:
            first_send(i - 1)
    first_send(strips - 1)

    for j in (1, 3, 0):
        hid_loads[j].wait()

        @pl.loop(0, strips - 1)
        def _(i):
            down_strip(j, i, wdq[i], 0)

        down_last(j)
        pair_copy(j).start()

    for copy in late_loads:
        copy.wait()

    for d in range(2):
        pair_copy(toward[d]).wait_recv()
    for p in range(PIECES):
        for d in range(2):
            h = 1 - d
            ring_out[d, 1, run_tiles(1, p)] = row_sum(toward[d], h * PIECES + p).astype(BF16)
            if p == 0:
                ring_out[d, 1, rotary_tiles(1)] = rotary_sum(toward[d], h).astype(BF16)
            send(d, ring_copy, 1, p)

    for d in range(2):
        ring_first_wait(d)
    for p in range(PIECES):
        for d in range(2):
            got = jnp.concatenate(
                [ring_in[d, 0, pl.ds(i * tiles + p * wide, wide)] for i in range(strips)], axis=0
            ).astype(F32)
            total = row_sum(toward[d], d * PIECES + p) + got
            ring_out[d, 2, run_tiles(2, p)] = total.astype(BF16)
            if p == 0:
                total = rotary_sum(toward[d], d) + ring_in[d, 0, rotary_tiles(0)].astype(F32)
                ring_out[d, 2, rotary_tiles(2)] = total.astype(BF16)
            send(d, ring_copy, 2, p)

    def totals(p):
        for h in range(2):
            ring_copy(1 - h, 1, p).wait_recv()
            ring_copy(h, 2, p).wait_recv()
            total = row_sum(0, h * PIECES + p)
            total += ring_in[1 - h, 1, run_tiles(1, p)].astype(F32) + ring_in[h, 2, run_tiles(2, p)].astype(F32)
            at = lat_rows(0, core, h, p)
            for first, end in ((0, q_tiles), (q_tiles, tiles)):
                part = total[first:end]
                squares = jnp.sum(jnp.sum(part * part, axis=0), axis=1, keepdims=True)
                scale = lax.rsqrt(squares / ((end - first) * LANES) + 1e-06)
                for k in range(first, end):
                    value = total[k] * scale * gain[k : k + 1, :]
                    lat[at, k * LANES : (k + 1) * LANES] = value.astype(BF16)
            forward(0, h, p).start()

    def sends(stage, p):
        for d in range(2):
            send(d, gather_copy, stage, p)

    def near(stage, p):
        for d in range(2):
            gather_wait(d, stage, p)
            forward(behind[d], (d, 1 - d)[stage], p).start()

    def far(p):
        for d in range(2):
            gather_wait(d, 2, p)
            forward(opposite, d, p).start()

    def ready(offsets, first, count):
        for p in range(first, first + count):
            for j in offsets:
                forward_wait(j, p)
        return piece_blocks(chip, block, offsets, first, count)

    pair_copy(0).wait_recv()
    totals(0)
    sends(0, 0)
    totals(1)
    sends(1, 0)
    totals(2)
    own = ready((0,), 0, 2)
    queries_in(own)
    keys_values_in(own)
    sends(0, 1)
    totals(3)
    sends(1, 1)
    own = ready((0,), 2, 2)
    queries_in(own)
    keys_values_in(own)
    sends(0, 2)
    near(0, 0)
    sends(1, 2)
    near(1, 0)
    sends(0, 3)
    near(0, 1)
    sends(1, 3)
    near(1, 1)
    near_rows = ready((1, 3), 0, 2)
    queries_in(near_rows)
    sends(2, 0)
    keys_values_in(near_rows)
    for h in range(2):
        total = rotary_sum(0, h)
        total += ring_in[1 - h, 1, rotary_tiles(1)].astype(F32) + ring_in[h, 2, rotary_tiles(2)].astype(F32)
        for g in range(2):
            a, b = lat_rows(0, core, h, 2 * g), lat_rows(0, core, h, 2 * g + 1)
            cosine = jnp.where(lane < ROPE, tab[0, a, :], tab[0, b, :])
            sine = jnp.where(lane < ROPE, tab[1, a, :], tab[1, b, :])
            turned = turn(total[g], cosine, sine)
            low = h * half + 2 * g * TILE
            keyrow[low : low + TILE, :] = turned
            keyrow[low + TILE : low + 2 * TILE, :] = pltpu.roll(turned, ROPE, 1)
    keybuf[...] = keyrow[...].T[:ROPE].astype(BF16)
    sends(2, 1)
    near(0, 2)
    sends(2, 2)
    near(1, 2)
    near(0, 3)
    sends(2, 3)
    near_rows = ready((1, 3), 2, 1)
    queries_in(near_rows)
    keys_values_in(near_rows)
    near(1, 3)
    far(0)
    near_rows = ready((1, 3), 3, 1)
    queries_in(near_rows)
    far(1)
    keys_values_in(near_rows)
    far(2)
    far_rows = ready((opposite,), 0, 2)
    queries_in(far_rows)
    far(3)
    keys_values_in(far_rows)

    remote(pair_out, pair_in, pair_s.at[0], pair_r.at[0], partner).wait_send()
    for d in range(2):
        drain(d, len(sent[d]))
    whole = lat.at[pl.ds(0, CHIPS * block)]
    remote(whole, whole, fw_s.at[0], fw_r.at[0, 0], partner).wait_send()
    for p in range(PIECES // 2, PIECES):
        forward_wait(opposite, p)


def store(q, kv, key, lat, wuq, wukv, tab, q_out, kv_out, key_out, qlast, kvlast, sem):
    _, chip, _ = place()
    block = q.shape[0] // (2 * CHIPS)
    last = piece_blocks(chip, block, (2,), 2, 2)
    pltpu.make_async_copy(key, key_out, sem.at[2]).start()
    early = [
        pl.ds(pl.multiple_of(lax.rem(chip + j, CHIPS) * 2 * block, 2 * block), 2 * block) for j in (0, 1, 3)
    ]
    for at in early + piece_blocks(chip, block, (2,), 0, 2):
        pltpu.make_async_copy(q.at[at], q_out.at[at], sem.at[0]).start()
        pltpu.make_async_copy(kv.at[at], kv_out.at[at], sem.at[1]).start()

    def put_q(b, column, values):
        qlast[b * (block // 4) : (b + 1) * (block // 4), pl.ds(column, LANES)] = values

    def put_kv(b, column, values):
        kvlast[b * (block // 4) : (b + 1) * (block // 4), pl.ds(column, values.shape[1])] = values

    def finish(src, dst, done):
        for b, at in enumerate(last):
            pltpu.make_async_copy(src.at[pl.ds(b * (block // 4), block // 4)], dst.at[at], done).start()

    up_keys_values(last, lat, wukv, put_kv, 2)
    finish(kvlast, kv_out, sem.at[1])
    up_queries(last, lat, wuq, tab, put_q, 2)
    finish(qlast, q_out, sem.at[0])
    pltpu.make_async_copy(q, q_out, sem.at[0]).wait()
    pltpu.make_async_copy(kv, kv_out, sem.at[1]).wait()
    pltpu.make_async_copy(key, key_out, sem.at[2]).wait()


def shards(hidden, w_dq, w_dkv, q_gain, kv_gain, w_uq, w_ukv):
    rows = hidden.shape[0]
    features, q_width = w_dq.shape
    w_dkv = w_dkv.T
    kv_width = kv_gain.shape[0]
    tiles = (q_width + kv_width) // LANES
    block = rows // (2 * CHIPS)
    table = jnp.asarray(rotary_tables(rows))
    dma = pltpu.SemaphoreType.DMA
    any_spec = pl.BlockSpec(memory_space=pl.ANY)
    vmem_spec = pl.BlockSpec(memory_space=pltpu.VMEM)
    shapes = ((rows, w_uq.shape[1]), (rows, w_ukv.shape[1]), (ROPE, block))
    flops = 2 * rows * (features * (q_width + w_dkv.shape[0]) + q_width * w_uq.shape[1] + kv_width * w_ukv.shape[1])
    pair_tiles = (block // TILE) * tiles + block // TILE // 2
    results = pl.pallas_call(
        kernel,
        out_shape=(
            *(pltpu.VMEM(shape, BF16) for shape in shapes),
            pltpu.VMEM((rows, q_width + kv_width), BF16),
            pltpu.VMEM(w_uq.shape, BF16),
            pltpu.VMEM(w_ukv.shape, BF16),
            pltpu.VMEM(table.shape, F32),
        ),
        in_specs=[any_spec] * 8,
        out_specs=(vmem_spec,) * 7,
        scratch_shapes=[
            pltpu.VMEM(hidden.shape, BF16),
            pltpu.VMEM((3, features, q_width // 3), BF16),
            pltpu.VMEM((kv_width + 2 * ROPE, features), BF16),
            pltpu.VMEM((tiles, LANES), F32),
            pltpu.VMEM((CHIPS, pair_tiles, TILE, LANES), F32),
            pltpu.VMEM((CHIPS, pair_tiles, TILE, LANES), BF16),
            pltpu.VMEM((CHIPS, pair_tiles, TILE, LANES), BF16),
            pltpu.VMEM((2, 3, PIECES * tiles + 2, TILE, LANES), BF16),
            pltpu.VMEM((2, 3, PIECES * tiles + 2, TILE, LANES), BF16),
            pltpu.VMEM((block, LANES), F32),
            dma((13,)),
            dma((4,)), dma((1,)), dma((CHIPS,)),
            dma((2, PIECES)), dma((2,)), dma((2, 2, PIECES)), dma((2, 3, PIECES)),
            dma((1,)), dma((CHIPS, PIECES)),
        ],
        compiler_params=pltpu.CompilerParams(
            collective_id=0, has_side_effects=True, vmem_limit_bytes=47_000_000
        ),
        cost_estimate=pl.CostEstimate(flops=flops, bytes_accessed=13_000_000, transcendentals=0),
    )(
        hidden, w_dq, w_dkv, q_gain.reshape(-1, LANES), kv_gain.reshape(-1, LANES), w_uq, w_ukv, table
    )
    queries, keys_values, rotary = pl.pallas_call(
        store,
        out_shape=tuple(jax.ShapeDtypeStruct(shape, BF16) for shape in shapes),
        in_specs=[vmem_spec] * 7,
        out_specs=(any_spec,) * 3,
        scratch_shapes=[
            pltpu.VMEM((block, w_uq.shape[1]), BF16),
            pltpu.VMEM((block, w_ukv.shape[1]), BF16),
            dma((3,)),
        ],
        compiler_params=pltpu.CompilerParams(vmem_limit_bytes=8 * 1024 * 1024),
        cost_estimate=pl.CostEstimate(flops=flops // 16, bytes_accessed=7_400_000, transcendentals=0),
    )(*results)
    return queries, keys_values, rotary.T


def solution(mesh):
    in_specs = (
        P("dp", "tensor"),
        P("tensor", None),
        P("tensor", None),
        P(),
        P(),
        P(None, "tensor"),
        P(None, "tensor"),
    )
    out_specs = (P("dp", "tensor"), P("dp", "tensor"), P(("dp", "tensor"), None))
    return jax.shard_map(shards, mesh=mesh, in_specs=in_specs, out_specs=out_specs, check_vma=False)
```

```python
import jax
import jax.numpy as jnp
import numpy as np
from jax import lax
from jax.experimental import pallas as pl
from jax.experimental.pallas import tpu as pltpu
from jax.sharding import PartitionSpec as P

NOPE = 128
ROPE = 64
CHIPS = 4
PIECES = 4
WINDOWS = (2, 3)
TILE = 16
LANES = 128
MESH = pl.DeviceIdType.MESH
F32 = jnp.float32
BF16 = jnp.bfloat16


def rotary_tables(count):
    half = ROPE // 2
    freqs = (50000.0 ** (-np.arange(half, dtype=np.float32) / half)).astype(np.float32)
    angle = np.arange(count, dtype=np.float32)[:, None] * freqs[None, :]
    cosine = np.cos(angle.astype(np.float64)).astype(np.float32)
    sine = np.sin(angle.astype(np.float64)).astype(np.float32)
    cosine = np.tile(cosine, (1, 4))
    sine = np.concatenate([-sine, sine, -sine, sine], axis=1)
    return np.stack([cosine, sine])


def lanes():
    return lax.broadcasted_iota(jnp.int32, (1, LANES), 1)


def turn(x, cosine, sine):
    low = lax.rem(lanes(), ROPE) < ROPE // 2
    swapped = jnp.where(low, pltpu.roll(x, LANES - ROPE // 2, 1), pltpu.roll(x, ROPE // 2, 1))
    return x * cosine + swapped * sine


def up_queries(blocks, lat, wuq, tab, put, steps):
    q_width = wuq.shape[0]
    pair = 2 * (NOPE + ROPE)
    heads = wuq.shape[1] // (steps * pair)
    lane = lanes()

    @pl.loop(0, steps)
    def _(i):
        start = pl.multiple_of(i * heads * pair, LANES)
        x = jnp.concatenate([lat[at, :q_width] for at in blocks], axis=0)
        cosine = jnp.concatenate([tab[0, at, :] for at in blocks], axis=0)
        sine = jnp.concatenate([tab[1, at, :] for at in blocks], axis=0)
        r = jnp.dot(x, wuq[:, pl.ds(start, heads * pair)], preferred_element_type=F32)
        for k in range(heads):
            x0 = r[:, k * pair : k * pair + 128]
            x1 = r[:, k * pair + 128 : k * pair + 256]
            x2 = r[:, k * pair + 256 : k * pair + 384]
            y1 = jnp.where(lane < ROPE, turn(x1, cosine, sine), x1)
            y2 = jnp.where(lane < ROPE, x2, turn(x2, cosine, sine))
            for n, y in enumerate((x0, y1, y2)):
                y = y.astype(BF16)
                row = 0
                for b, at in enumerate(blocks):
                    put(b, pl.multiple_of(start + k * pair + n * LANES, LANES), y[row : row + at.size])
                    row += at.size


def up_keys_values(blocks, lat, wukv, put, steps):
    q_width = lat.shape[1] - wukv.shape[0]
    width = wukv.shape[1] // steps

    @pl.loop(0, steps)
    def _(i):
        start = pl.multiple_of(i * width, LANES)
        x = jnp.concatenate([lat[at, q_width:] for at in blocks], axis=0)
        y = jnp.dot(x, wukv[:, pl.ds(start, width)], preferred_element_type=F32).astype(BF16)
        row = 0
        for b, at in enumerate(blocks):
            put(b, start, y[row : row + at.size])
            row += at.size


def place():
    me = lax.axis_index("tensor")
    chip = me // 2
    core = me - 2 * chip
    return me, chip, core


def piece_blocks(chip, block, offsets, first, count):
    size = count * TILE
    return [
        pl.ds(pl.multiple_of((lax.rem(chip + j, CHIPS) * 2 + c) * block + h * (block // 2) + first * TILE, TILE), size)
        for j in offsets for c in range(2) for h in range(2)
    ]


def kernel(
    hidden, w_dq, w_dkv, q_gain, kv_gain, w_uq, w_ukv, table,
    qbuf, kvbuf, keybuf, lat, wuq, wukv, tab,
    hid, wdq, wdkv, gain, acc, pair_out, pair_in, ring_out, ring_in, keyrow,
    load_sem, first_r, pair_s, pair_r, ring_s, rs_first_r, rs_r, ag_r, fw_s, fw_r,
):
    rows = hid.shape[0]
    q_width = w_uq.shape[0]
    kv_width = w_ukv.shape[0]
    latent_width = q_width + kv_width
    q_tiles, tiles = q_width // LANES, latent_width // LANES
    block = rows // (2 * CHIPS)
    half = block // 2
    row_tiles = block // TILE
    strips = 4
    wide = tiles // strips
    me, chip, core = place()
    partner = me + 1 - 2 * core

    def chip_at(j):
        return lax.rem(chip + j, CHIPS)

    neighbour = (chip_at(1) * 2 + core, chip_at(CHIPS - 1) * 2 + core)
    toward = (1, CHIPS - 1)
    behind = (CHIPS - 1, 1)
    opposite = 2

    def load(i, src, dst):
        return pltpu.make_async_copy(src, dst, load_sem.at[i])

    def chip_rows(j):
        return pl.ds(pl.multiple_of(chip_at(j) * 2 * block, 2 * block), 2 * block)

    width = wide * LANES
    hid_loads = [load(j, hidden.at[chip_rows(j)], hid.at[chip_rows(j)]) for j in range(CHIPS)]
    strip_loads = [load(4 + i, w_dq.at[:, pl.ds(i * width, width)], wdq.at[i]) for i in range(strips - 1)]
    strip_loads.append(load(7, w_dkv, wdkv.at[pl.ds(0, kv_width + ROPE)]))
    late_loads = [
        load(8, q_gain, gain.at[pl.ds(0, q_tiles)]), load(9, kv_gain, gain.at[pl.ds(q_tiles, tiles - q_tiles)]),
        load(10, table, tab), load(11, w_ukv, wukv), load(12, w_uq, wuq),
    ]
    barrier = pltpu.get_barrier_semaphore()
    for device in (*neighbour, partner):
        pl.semaphore_signal(barrier, inc=1, device_id={"tensor": device}, device_id_type=MESH)
    hid_loads[opposite].start()
    for copy in strip_loads[:2]:
        copy.start()
    wdkv[kv_width + ROPE :, :] = jnp.zeros((ROPE, wdkv.shape[1]), BF16)

    def remote(src, dst, send, recv, device):
        return pltpu.make_async_remote_copy(
            src_ref=src, dst_ref=dst, send_sem=send, recv_sem=recv,
            device_id={"tensor": device}, device_id_type=MESH,
        )

    rotary_at = strips * row_tiles * wide
    lane = lanes()

    def down_strip(j, i, weights, depth):
        base = chip_at(j) * 2 * block
        other = pl.ds(pl.multiple_of(base + (1 - core) * block, block), block)
        own = pl.ds(pl.multiple_of(base + core * block, block), block)
        x = jnp.concatenate([hid[other, :], hid[own, :]], axis=0)
        r = lax.dot_general(x, weights, (((1,), (depth,)), ((), ())), preferred_element_type=F32)
        first = i * row_tiles * wide
        for t in range(row_tiles):
            for c in range(wide):
                cols = slice(c * LANES, (c + 1) * LANES)
                low = t * TILE
                pair_out[j, first + t * wide + c] = r[low : low + TILE, cols].astype(BF16)
                acc[j, first + t * wide + c] = r[block + low : block + low + TILE, cols]

    def down_rotary(j):
        base = chip_at(j) * 2 * block
        other = pl.ds(pl.multiple_of(base + (1 - core) * block, block), block)
        own = pl.ds(pl.multiple_of(base + core * block, block), block)
        x = jnp.concatenate([hid[other, :], hid[own, :]], axis=0)
        r = lax.dot_general(x, wdkv[kv_width:, :], (((1,), (1,)), ((), ())), preferred_element_type=F32)
        for side in range(2):
            for g in range(row_tiles // 2):
                low = side * block + g * 2 * TILE
                a, b = r[low : low + TILE], r[low + TILE : low + 2 * TILE]
                packed = jnp.where(lane < ROPE, a, pltpu.roll(b, ROPE, 1))
                if side == 0:
                    pair_out[j, rotary_at + g] = packed.astype(BF16)
                else:
                    acc[j, rotary_at + g] = packed

    def down_last(j):
        down_strip(j, strips - 1, wdkv[:kv_width, :], 1)
        down_rotary(j)

    def first_copy(i):
        size = row_tiles * wide
        at = pl.ds(i * size, size + (row_tiles // 2 if i == strips - 1 else 0))
        return remote(
            pair_out.at[opposite, at], pair_in.at[opposite, at], pair_s.at[0], first_r.at[i], partner
        )

    def pair_copy(j):
        return remote(pair_out.at[j], pair_in.at[j], pair_s.at[0], pair_r.at[0 if j == 0 else 1], partner)

    def strip_sum(j, i, t, count):
        at = pl.ds((i * row_tiles + t) * wide, count * wide)
        return acc[j, at] + pair_in[j, at].astype(F32)

    def row_sum(j, t):
        return jnp.concatenate([strip_sum(j, i, t, 1) for i in range(strips)], axis=0)

    def rotary_sum(j, h):
        at = pl.ds(rotary_at + h * 2, 2)
        return acc[j, at] + pair_in[j, at].astype(F32)

    def run(stage, p):
        if stage == 0:
            return pl.ds(p * tiles, tiles + (2 if p == PIECES - 1 else 0))
        return pl.ds(0, tiles + 2) if p == 0 else pl.ds(p * tiles + 2, tiles)

    def run_tiles(stage, p):
        return pl.ds(run(stage, p).start, tiles)

    def rotary_tiles(stage):
        return pl.ds(PIECES * tiles if stage == 0 else tiles, 2)

    def ring_copy(d, stage, p, n=0):
        at = run(stage, p)
        recv = rs_first_r.at[0] if stage == 0 else rs_r.at[p]
        return remote(
            ring_out.at[d, stage, at], ring_in.at[d, stage, at], ring_s.at[d, n % PIECES], recv, neighbour[d]
        )

    def tiles_wait(count, recv):
        at = pair_in.at[0, pl.ds(0, count)]
        remote(at, at, pair_s.at[0], recv, partner).wait_recv()

    def lat_rows(j, c, h, p):
        start = (chip_at(j) * 2 + c) * block + h * half + p * TILE
        return pl.ds(pl.multiple_of(start, TILE), TILE)

    def gather_copy(d, stage, p, n):
        j = (0, 0, behind[d])[stage]
        h = (d, 1 - d, d)[stage]
        at = lat.at[lat_rows(j, core, h, p)]
        return remote(at, at, ring_s.at[d, n % PIECES], ag_r.at[stage, p], neighbour[d])

    def rows_wait(count, recv):
        at = lat.at[pl.ds(0, count)]
        remote(at, at, fw_s.at[0], recv, partner).wait_recv()

    def forward(j, h, p):
        at = lat.at[lat_rows(j, core, h, p)]
        group = ((0, 0, 1, 1), (2, 2, 3, 3), (4, 4, 5, 5), (2, 2, 3, 3))[j][p]
        return remote(at, at, fw_s.at[0], fw_r.at[group], partner)

    sent = ([], [])

    done = [0, 0]

    def drain(d, end):
        for copy in sent[d][done[d] : end]:
            copy.wait_send()
        done[d] = end

    def send(d, make, *which):
        n = len(sent[d])
        if n >= PIECES:
            drain(d, n - WINDOWS[0 if n < 3 * PIECES else 1] + 1)
        copy = make(d, *which, n)
        copy.start()
        sent[d].append(copy)

    def queries_in(blocks):
        def put(b, column, values):
            qbuf[blocks[b], pl.ds(column, LANES)] = values
        up_queries(blocks, lat, wuq, tab, put, 1)

    def keys_values_in(blocks):
        def put(b, column, values):
            kvbuf[blocks[b], pl.ds(column, values.shape[1])] = values
        up_keys_values(blocks, lat, wukv, put, 1)

    def first_send(i):
        first_copy(i).wait_recv()
        for d in range(2):
            t = d * PIECES
            ring_out[d, 0, pl.ds(i * tiles, tiles)] = strip_sum(opposite, i, t, PIECES).astype(BF16)
            if i == strips - 1:
                ring_out[d, 0, rotary_tiles(0)] = rotary_sum(opposite, d).astype(BF16)
            send(d, ring_copy, 0, i)

    hid_loads[opposite].wait()
    for i in range(strips):
        strip_loads[i].wait()
        if i == 0:
            for copy in (*strip_loads[2:], *(hid_loads[j] for j in (1, 3, 0))):
                copy.start()
        if i < strips - 1:
            down_strip(opposite, i, wdq[i], 0)
        else:
            down_last(opposite)
        if i == 0:
            pl.semaphore_wait(barrier, 3)
        first_copy(i).start()
        if i == 1:
            for copy in late_loads:
                copy.start()
        if i > 0:
            first_send(i - 1)
    first_send(strips - 1)

    for j in (1, 3, 0):
        hid_loads[j].wait()

        @pl.loop(0, strips - 1)
        def _(i):
            down_strip(j, i, wdq[i], 0)

        down_last(j)
        pair_copy(j).start()

    for copy in late_loads:
        copy.wait()

    two = pair_in.at[pl.ds(0, 2)]
    remote(two, two, pair_s.at[0], pair_r.at[1], partner).wait_recv()
    for p in range(PIECES):
        for d in range(2):
            h = 1 - d
            ring_out[d, 1, run_tiles(1, p)] = row_sum(toward[d], h * PIECES + p).astype(BF16)
            if p == 0:
                ring_out[d, 1, rotary_tiles(1)] = rotary_sum(toward[d], h).astype(BF16)
            send(d, ring_copy, 1, p)

    tiles_wait(2 * (PIECES * tiles + 2), rs_first_r.at[0])
    for p in range(PIECES):
        for d in range(2):
            got = jnp.concatenate(
                [ring_in[d, 0, pl.ds(i * tiles + p * wide, wide)] for i in range(strips)], axis=0
            ).astype(F32)
            total = row_sum(toward[d], d * PIECES + p) + got
            ring_out[d, 2, run_tiles(2, p)] = total.astype(BF16)
            if p == 0:
                total = rotary_sum(toward[d], d) + ring_in[d, 0, rotary_tiles(0)].astype(F32)
                ring_out[d, 2, rotary_tiles(2)] = total.astype(BF16)
            send(d, ring_copy, 2, p)

    def totals(p):
        tiles_wait(4 * (tiles + (2 if p == 0 else 0)), rs_r.at[p])
        for h in range(2):
            total = row_sum(0, h * PIECES + p)
            total += ring_in[1 - h, 1, run_tiles(1, p)].astype(F32) + ring_in[h, 2, run_tiles(2, p)].astype(F32)
            at = lat_rows(0, core, h, p)
            for first, end in ((0, q_tiles), (q_tiles, tiles)):
                part = total[first:end]
                squares = jnp.sum(jnp.sum(part * part, axis=0), axis=1, keepdims=True)
                scale = lax.rsqrt(squares / ((end - first) * LANES) + 1e-06)
                for k in range(first, end):
                    value = total[k] * scale * gain[k : k + 1, :]
                    lat[at, k * LANES : (k + 1) * LANES] = value.astype(BF16)
            forward(0, h, p).start()

    def sends(stage, p):
        for d in range(2):
            send(d, gather_copy, stage, p)

    def near(stage, p):
        rows_wait(2 * TILE, ag_r.at[stage, p])
        for d in range(2):
            forward(behind[d], (d, 1 - d)[stage], p).start()

    def far(p):
        rows_wait(2 * TILE, ag_r.at[2, p])
        for d in range(2):
            forward(opposite, d, p).start()

    def ready(group, offsets, first, count):
        rows_wait(len(offsets) * count * 2 * TILE, fw_r.at[group])
        return piece_blocks(chip, block, offsets, first, count)

    pair_copy(0).wait_recv()
    totals(0)
    sends(0, 0)
    totals(1)
    sends(1, 0)
    totals(2)
    own = ready(0, (0,), 0, 2)
    queries_in(own)
    keys_values_in(own)
    sends(0, 1)
    totals(3)
    sends(1, 1)
    own = ready(1, (0,), 2, 2)
    queries_in(own)
    keys_values_in(own)
    sends(0, 2)
    near(0, 0)
    sends(1, 2)
    near(1, 0)
    sends(0, 3)
    near(0, 1)
    sends(1, 3)
    sends(2, 0)
    near(1, 1)
    sends(2, 1)
    near_rows = ready(2, (1, 3), 0, 2)
    queries_in(near_rows)
    near(0, 2)
    sends(2, 2)
    near(1, 2)
    near(0, 3)
    sends(2, 3)
    near(1, 3)
    keys_values_in(near_rows)
    for h in range(2):
        total = rotary_sum(0, h)
        total += ring_in[1 - h, 1, rotary_tiles(1)].astype(F32) + ring_in[h, 2, rotary_tiles(2)].astype(F32)
        for g in range(2):
            a, b = lat_rows(0, core, h, 2 * g), lat_rows(0, core, h, 2 * g + 1)
            cosine = jnp.where(lane < ROPE, tab[0, a, :], tab[0, b, :])
            sine = jnp.where(lane < ROPE, tab[1, a, :], tab[1, b, :])
            turned = turn(total[g], cosine, sine)
            low = h * half + 2 * g * TILE
            keyrow[low : low + TILE, :] = turned
            keyrow[low + TILE : low + 2 * TILE, :] = pltpu.roll(turned, ROPE, 1)
    keybuf[...] = keyrow[...].T[:ROPE].astype(BF16)
    near_rows = ready(3, (1, 3), 2, 2)
    queries_in(near_rows)
    far(0)
    far(1)
    keys_values_in(near_rows)
    far(2)
    far_rows = ready(4, (opposite,), 0, 2)
    queries_in(far_rows)
    far(3)
    keys_values_in(far_rows)

    remote(pair_out, pair_in, pair_s.at[0], pair_r.at[0], partner).wait_send()
    for d in range(2):
        drain(d, len(sent[d]))
    whole = lat.at[pl.ds(0, CHIPS * block)]
    remote(whole, whole, fw_s.at[0], fw_r.at[0], partner).wait_send()
    ready(5, (opposite,), 2, 2)


def store(q, kv, key, lat, wuq, wukv, tab, q_out, kv_out, key_out, qlast, kvlast, sem):
    _, chip, _ = place()
    block = q.shape[0] // (2 * CHIPS)
    last = piece_blocks(chip, block, (2,), 2, 2)
    pltpu.make_async_copy(key, key_out, sem.at[2]).start()
    early = [
        pl.ds(pl.multiple_of(lax.rem(chip + j, CHIPS) * 2 * block, 2 * block), 2 * block) for j in (0, 1, 3)
    ]
    for at in early + piece_blocks(chip, block, (2,), 0, 2):
        pltpu.make_async_copy(q.at[at], q_out.at[at], sem.at[0]).start()
        pltpu.make_async_copy(kv.at[at], kv_out.at[at], sem.at[1]).start()

    def put_q(b, column, values):
        qlast[b * (block // 4) : (b + 1) * (block // 4), pl.ds(column, LANES)] = values

    def put_kv(b, column, values):
        kvlast[b * (block // 4) : (b + 1) * (block // 4), pl.ds(column, values.shape[1])] = values

    def finish(src, dst, done):
        for b, at in enumerate(last):
            pltpu.make_async_copy(src.at[pl.ds(b * (block // 4), block // 4)], dst.at[at], done).start()

    up_keys_values(last, lat, wukv, put_kv, 2)
    finish(kvlast, kv_out, sem.at[1])
    up_queries(last, lat, wuq, tab, put_q, 2)
    finish(qlast, q_out, sem.at[0])
    pltpu.make_async_copy(q, q_out, sem.at[0]).wait()
    pltpu.make_async_copy(kv, kv_out, sem.at[1]).wait()
    pltpu.make_async_copy(key, key_out, sem.at[2]).wait()


def shards(hidden, w_dq, w_dkv, q_gain, kv_gain, w_uq, w_ukv):
    rows = hidden.shape[0]
    features, q_width = w_dq.shape
    w_dkv = w_dkv.T
    kv_width = kv_gain.shape[0]
    tiles = (q_width + kv_width) // LANES
    block = rows // (2 * CHIPS)
    table = jnp.asarray(rotary_tables(rows))
    dma = pltpu.SemaphoreType.DMA
    any_spec = pl.BlockSpec(memory_space=pl.ANY)
    vmem_spec = pl.BlockSpec(memory_space=pltpu.VMEM)
    shapes = ((rows, w_uq.shape[1]), (rows, w_ukv.shape[1]), (ROPE, block))
    flops = 2 * rows * (features * (q_width + w_dkv.shape[0]) + q_width * w_uq.shape[1] + kv_width * w_ukv.shape[1])
    pair_tiles = (block // TILE) * tiles + block // TILE // 2
    results = pl.pallas_call(
        kernel,
        out_shape=(
            *(pltpu.VMEM(shape, BF16) for shape in shapes),
            pltpu.VMEM((rows, q_width + kv_width), BF16),
            pltpu.VMEM(w_uq.shape, BF16),
            pltpu.VMEM(w_ukv.shape, BF16),
            pltpu.VMEM(table.shape, F32),
        ),
        in_specs=[any_spec] * 8,
        out_specs=(vmem_spec,) * 7,
        scratch_shapes=[
            pltpu.VMEM(hidden.shape, BF16),
            pltpu.VMEM((3, features, q_width // 3), BF16),
            pltpu.VMEM((kv_width + 2 * ROPE, features), BF16),
            pltpu.VMEM((tiles, LANES), F32),
            pltpu.VMEM((CHIPS, pair_tiles, TILE, LANES), F32),
            pltpu.VMEM((CHIPS, pair_tiles, TILE, LANES), BF16),
            pltpu.VMEM((CHIPS, pair_tiles, TILE, LANES), BF16),
            pltpu.VMEM((2, 3, PIECES * tiles + 2, TILE, LANES), BF16),
            pltpu.VMEM((2, 3, PIECES * tiles + 2, TILE, LANES), BF16),
            pltpu.VMEM((block, LANES), F32),
            dma((13,)),
            dma((4,)), dma((1,)), dma((2,)),
            dma((2, PIECES)), dma((1,)), dma((PIECES,)), dma((3, PIECES)),
            dma((1,)), dma((6,)),
        ],
        compiler_params=pltpu.CompilerParams(
            collective_id=0, has_side_effects=True, vmem_limit_bytes=47_000_000
        ),
        cost_estimate=pl.CostEstimate(flops=flops, bytes_accessed=13_000_000, transcendentals=0),
    )(
        hidden, w_dq, w_dkv, q_gain.reshape(-1, LANES), kv_gain.reshape(-1, LANES), w_uq, w_ukv, table
    )
    queries, keys_values, rotary = pl.pallas_call(
        store,
        out_shape=tuple(jax.ShapeDtypeStruct(shape, BF16) for shape in shapes),
        in_specs=[vmem_spec] * 7,
        out_specs=(any_spec,) * 3,
        scratch_shapes=[
            pltpu.VMEM((block, w_uq.shape[1]), BF16),
            pltpu.VMEM((block, w_ukv.shape[1]), BF16),
            dma((3,)),
        ],
        compiler_params=pltpu.CompilerParams(vmem_limit_bytes=8 * 1024 * 1024),
        cost_estimate=pl.CostEstimate(flops=flops // 16, bytes_accessed=7_400_000, transcendentals=0),
    )(*results)
    return queries, keys_values, rotary.T


def solution(mesh):
    in_specs = (
        P("dp", "tensor"),
        P("tensor", None),
        P("tensor", None),
        P(),
        P(),
        P(None, "tensor"),
        P(None, "tensor"),
    )
    out_specs = (P("dp", "tensor"), P("dp", "tensor"), P(("dp", "tensor"), None))
    return jax.shard_map(shards, mesh=mesh, in_specs=in_specs, out_specs=out_specs, check_vma=False)
```
